256 devices in a mesh: node: 8 (over z), expert: 16 (over x, y), column: 2 (over core).
Axes of the slice: x: 4, y: 4, z: 8, core: 2. Of those that a mesh axis runs over, the one named last changes fastest.
Arguments:
- slot_grads: bfloat16 [128, 768, 2048], P(('node', 'expert'), None, 'column'), may hold values from -8 to 8
- slot_tokens: int32 [128], replicated, may hold values from 16 to 511
- old_slots: int32 [128], replicated, may hold values from 0 to 79, as said below
- owner_chip: int32 [128], replicated, may hold values from 0 to 127, each once
- momentum: bfloat16 [128, 768, 2048], P(('node', 'expert'), None, 'column'), may hold values from -3 to 3
- master: float32 [128, 768, 2048], P(('node', 'expert'), None, 'column'), may hold values from -0.5 to 0.5
- new_slots: int32 [128], replicated, may hold values from 0 to 79, as said below
Outputs:
- new_momentum: bfloat16 [128, 768, 2048], P(('node', 'expert'), None, 'column')
- new_master: float32 [128, 768, 2048], P(('node', 'expert'), None, 'column')
- new_slot_weights: bfloat16 [128, 768, 2048], P(('node', 'expert'), None, 'column')
The draws below stay inside these ranges and needn't reach their ends.
Inputs may be any that keep to these rules, and one draw needn't show every extreme that they name: `old_slots`: every expert 0 .. 79 is held by 1 to 4 slots, and some expert by exactly 4. `new_slots`: every expert 0 .. 79 is held by 1 to 4 slots, and some expert by exactly 4. Each chip position appears once; owner_chip[e] owns expert e for e below 80, and the chips named at 80 and beyond own none.
All inputs are finite; a program needn't handle non-finite values.
Results may differ from the reference program's by a relative error of at most 0.0023.
Values may be sent and summed in bfloat16 or wider, within the bound.
A program may use at most 128 MiB of HBM per device.

```python
import math
import jax
import jax.numpy as jnp
from jax import lax

D = 2048
FF = 768
ITERS = 2
CHIPS = 128
SLOTS = 128
EXPERTS = 80


spike_levels = (0.92, 0.55, 0.32, 0.18)


def slot_layout(key):
    base = jnp.arange(EXPERTS, dtype=jnp.int32)
    heavy = jax.random.randint(jax.random.fold_in(key, 1), (), 0, EXPERTS).astype(jnp.int32)
    copies = jnp.tile(base, 3)
    ranks = jax.random.permutation(jax.random.fold_in(key, 2), 3 * EXPERTS).astype(jnp.int32)
    scores = jnp.where(copies == heavy, ranks - 3 * EXPERTS, ranks)
    ordering = jnp.argsort(scores, stable=True)
    extras = copies[ordering[:SLOTS - EXPERTS]]
    layout = jnp.concatenate([base, extras])
    shuffle = jax.random.permutation(jax.random.fold_in(key, 3), SLOTS)
    return layout[shuffle].astype(jnp.int32)


def draw_old_slots(key, part):
    return slot_layout(jax.random.fold_in(key, 11))


def draw_new_slots(key, part):
    return slot_layout(jax.random.fold_in(key, 12))


def draw_slot_grads(key, part):
    layout = slot_layout(jax.random.fold_in(key, 11))
    noise = jax.random.normal(jax.random.fold_in(key, 21), (SLOTS, FF, D), jnp.float32)
    spike_total = len(spike_levels)
    left = jnp.clip(jax.random.normal(jax.random.fold_in(key, 31), (EXPERTS, FF, spike_total), jnp.float32), -3.0, 3.0)
    right = jnp.clip(jax.random.normal(jax.random.fold_in(key, 32), (EXPERTS, spike_total, D), jnp.float32), -3.0, 3.0)
    jitter = jax.random.uniform(jax.random.fold_in(key, 33), (SLOTS, spike_total), jnp.float32, 0.7, 1.3)
    levels = jnp.array(spike_levels, jnp.float32)[None, :] * jitter
    slot_left = left[layout] * levels[:, None, :]
    spikes = jnp.einsum('sfk,skd->sfd', slot_left, right[layout], precision=lax.Precision.HIGHEST)
    values = jnp.clip(noise + spikes, -8.0, 8.0)
    return values.astype(jnp.bfloat16)


def set_ends(values, own_key, low, top_value):
    spot = [jax.random.randint(jax.random.fold_in(own_key, axis), (), 0, length) for axis, length in enumerate(values.shape)]
    main_axis = values.shape.index(max(values.shape))
    next_to = spot[:main_axis] + [(spot[main_axis] + 1) % values.shape[main_axis]] + spot[main_axis + 1:]
    return values.at[tuple(spot)].set(low).at[tuple(next_to)].set(top_value)


def steps_of(stream_key, extent, cuts, least, high):
    def one(axis_at, blocks):
        heights = jax.random.uniform(jax.random.fold_in(jax.random.fold_in(stream_key, 6), axis_at), (blocks,), jnp.float32, least / len(cuts), high / len(cuts))
        return jnp.repeat(jnp.exp(heights), extent[axis_at] // blocks).reshape((-1,) + (1,) * (len(extent) - axis_at - 1))

    gain = one(*cuts[0])
    for cut in cuts[1:]:
        gain = gain * one(*cut)
    return gain


def gaussian(own_key, shape, deviation, limit, pieces=(), kind=jnp.bfloat16):
    result = deviation * jax.random.normal(own_key, shape, jnp.float32)
    if pieces:
        result = result * steps_of(own_key, shape, pieces, -0.22, 0.18)
    return jnp.clip(result, -limit, limit).astype(kind)


def setup_inputs(seed: int = 0) -> dict:
    key_of = jax.random.split(jax.random.key(seed), 8)
    slot_grads = draw_slot_grads(jax.random.fold_in(key_of[7], 71), 0)
    slot_tokens = set_ends(jax.random.randint(key_of[1], (SLOTS,), 16, 512), jax.random.fold_in(key_of[1], 1), 16, 511).astype(jnp.int32)
    old_slots = draw_old_slots(jax.random.fold_in(key_of[7], 71), 0)
    owner_chip = jax.random.permutation(key_of[3], CHIPS).astype(jnp.int32)
    momentum = gaussian(key_of[4], (CHIPS, FF, D), 0.5, 3.0, ((0, 128), (2, 2)))
    master = gaussian(key_of[5], (CHIPS, FF, D), (D // 16) ** -0.5, 0.5, ((0, 128), (2, 2)), jnp.float32)
    new_slots = draw_new_slots(jax.random.fold_in(key_of[7], 71), 0)
    return dict(slot_grads=slot_grads, slot_tokens=slot_tokens, old_slots=old_slots, owner_chip=owner_chip, momentum=momentum, master=master, new_slots=new_slots)


coef_a = 3.4445
coef_b = -4.775
coef_c = 2.0315
momentum_beta = 0.95
learn_rate = 1.0
weight_decay = 0.1
epsilon = 1e-07
highest = lax.Precision.HIGHEST

def mixing_table(slot_tokens, old_slots, owner_chip):
    chip_ids = lax.iota(jnp.int32, CHIPS)
    matches = (owner_chip[None, :] == chip_ids[:, None]) & (chip_ids[None, :] < EXPERTS)
    owned_expert = lax.optimization_barrier(jnp.sum(jnp.where(matches, chip_ids[None, :], 0), axis=1))
    holders = jnp.any(matches, axis=1)
    picked = (old_slots[None, :] == owned_expert[:, None]) & holders[:, None]
    counts = jnp.where(picked, slot_tokens[None, :].astype(jnp.float32), jnp.float32(0.0))
    totals = jnp.maximum(lax.optimization_barrier(jnp.sum(counts, axis=1, keepdims=True)), jnp.float32(1.0))
    return counts / totals

def orthogonal_update(blocks):
    grad_block, moment_block, master_block = blocks
    moment = momentum_beta * moment_block.astype(jnp.float32) + grad_block
    nesterov = grad_block + momentum_beta * moment
    squares = jnp.sum(nesterov * nesterov)
    norm_scale = 1.0 / (jnp.sqrt(squares) + epsilon)
    iterate = nesterov * norm_scale
    for iteration in range(ITERS):
        gram_matrix = jnp.dot(iterate, iterate.T, precision=highest, preferred_element_type=jnp.float32)
        polynomial = coef_b * gram_matrix + coef_c * jnp.dot(gram_matrix, gram_matrix, precision=highest, preferred_element_type=jnp.float32)
        iterate = coef_a * iterate + jnp.dot(polynomial, iterate, precision=highest, preferred_element_type=jnp.float32)
    step_scale = learn_rate * 0.2 * math.sqrt(max(FF, D))
    master_new = (1.0 - learn_rate * weight_decay) * master_block - step_scale * iterate
    return (moment.astype(jnp.bfloat16), master_new)

def reference(slot_grads, slot_tokens, old_slots, owner_chip, momentum, master, new_slots):
    mixing = mixing_table(slot_tokens, old_slots, owner_chip)
    flattened = slot_grads.reshape(SLOTS, FF * D).astype(jnp.float32)
    grads = jnp.dot(mixing, flattened, precision=highest, preferred_element_type=jnp.float32).reshape(CHIPS, FF, D)
    new_momentum, new_master = lax.map(orthogonal_update, (grads, momentum, master))
    weights = new_master.astype(jnp.bfloat16)
    sources = owner_chip[new_slots]
    new_slot_weights = weights[sources]
    return (new_momentum, new_master, new_slot_weights)
```

```python
import math

import jax
import jax.numpy as jnp
from jax import lax
from jax.experimental import pallas as pl
from jax.experimental.pallas import tpu as pltpu
from jax.sharding import PartitionSpec as P

D = 2048
FF = 768
CHIPS = 128
EXPERTS = 80
NODES = 8
PLANE = 16
ROWS = FF // PLANE
FINE = 16
COLS = D // 2 // NODES

coef_a = 3.4445
coef_b = -4.775
coef_c = 2.0315
momentum_beta = 0.95
learn_rate = 1.0
weight_decay = 0.1
epsilon = 1e-07

MESH = pl.DeviceIdType.MESH


def position():
    return lax.axis_index("node"), lax.axis_index("expert"), lax.axis_index("column")


def partner(step, node, spot):
    to_node = lax.rem(node + lax.rem(step, 8), 8)
    to_x = lax.rem(spot // 4 + lax.rem(step // 8, 4), 4)
    to_y = lax.rem(lax.rem(spot, 4) + step // 32, 4)
    return to_node, to_x * 4 + to_y


def block_of(ref, node, spot, height=ROWS):
    rows = pl.ds(pl.multiple_of(spot * height, height), height)
    cols = pl.ds(pl.multiple_of(node * COLS, COLS), COLS)
    return ref.at[rows, cols]


def greet_all(node, spot, core):
    barrier = pltpu.get_barrier_semaphore()

    def greet(step, carry):
        to_node, to_spot = partner(step, node, spot)
        pl.semaphore_signal(
            barrier, inc=1, device_id=(to_node, to_spot, core), device_id_type=MESH
        )
        return carry

    lax.fori_loop(1, CHIPS, greet, 0)
    pl.semaphore_wait(barrier, CHIPS - 1)


def spread(source, landing, send_sem, recv_sem, node, spot, core):
    me = node * PLANE + spot

    def send(step, carry):
        to_node, to_spot = partner(step, node, spot)
        pltpu.make_async_remote_copy(
            block_of(source, to_node, to_spot),
            landing.at[me],
            send_sem,
            recv_sem,
            device_id=(to_node, to_spot, core),
            device_id_type=MESH,
        ).start()
        return carry

    lax.fori_loop(1, CHIPS, send, 0)
    landing[me] = block_of(source, node, spot)[...]


def send_block(pieces, target, send_sem, recv_sem, step, node, spot, core):
    to_node, to_spot = partner(step, node, spot)
    pltpu.make_async_remote_copy(
        pieces.at[to_node * PLANE + to_spot],
        block_of(target, node, spot, pieces.shape[1]),
        send_sem,
        recv_sem,
        device_id=(to_node, to_spot, core),
        device_id_type=MESH,
    ).start()


def whole_wait(buffer, send_sem, recv_sem, node, spot, core, which):
    rest = buffer.at[pl.ds(0, CHIPS - 1)]
    copy = pltpu.make_async_remote_copy(
        rest, rest, send_sem, recv_sem, device_id=(node, spot, core), device_id_type=MESH
    )
    if which == "send":
        copy.wait_send()
    else:
        copy.wait_recv()


def tables(tokens_ref, old_ref, owner_ref, index_ref, weight_ref):
    shape = (CHIPS, CHIPS)
    across = lax.broadcasted_iota(jnp.int32, shape, 1)
    down = lax.broadcasted_iota(jnp.int32, shape, 0)
    owner = jnp.broadcast_to(owner_ref[...], shape).T
    match = (owner == across) & (down < EXPERTS)
    owned = jnp.sum(jnp.where(match, down + 1, 0), axis=0, keepdims=True) - 1
    old = jnp.broadcast_to(old_ref[...], shape).T
    tokens = jnp.broadcast_to(tokens_ref[...], shape).T
    picked = old == owned
    total = jnp.sum(jnp.where(picked, tokens, 0), axis=0, keepdims=True)
    total = jnp.maximum(total.astype(jnp.float32), 1.0)
    for k in range(4):
        first = jnp.min(jnp.where(picked, down, CHIPS), axis=0, keepdims=True)
        here = down == first
        count = jnp.sum(jnp.where(here, tokens, 0), axis=0, keepdims=True)
        weight_ref[k : k + 1, :] = count.astype(jnp.float32) / total
        index_ref[k : k + 1, :] = jnp.where(first < CHIPS, first, 0)
        picked = picked & jnp.logical_not(here)


def grads_kernel(
    grads_ref, tokens_ref, old_ref, owner_ref, out_ref, rest_ref,
    local, landing, pieces, rests, index_v, weight_v, index_s, weight_s,
    copy_sems, sems,
):
    node, spot, core = position()
    me = node * PLANE + spot
    load = pltpu.make_async_copy(grads_ref.at[0], local, copy_sems.at[0])
    load.start()
    greet_all(node, spot, core)
    load.wait()
    spread(local, landing, sems.at[0], sems.at[1], node, spot, core)
    tables(tokens_ref, old_ref, owner_ref, index_v, weight_v)
    to_smem = pltpu.make_async_copy(index_v, index_s, copy_sems.at[1])
    to_smem.start()
    to_smem2 = pltpu.make_async_copy(weight_v, weight_s, copy_sems.at[2])
    to_smem2.start()
    to_smem.wait()
    to_smem2.wait()
    whole_wait(landing, sems.at[0], sems.at[1], node, spot, core, "recv")

    def combine(step):
        to_node, to_spot = partner(step, node, spot)
        chip = to_node * PLANE + to_spot
        total = landing[index_s[0, chip]].astype(jnp.float32) * weight_s[0, chip]
        for k in range(1, 4):
            total += landing[index_s[k, chip]].astype(jnp.float32) * weight_s[k, chip]
        near = total.astype(jnp.bfloat16)
        pieces[chip] = near
        rests[chip] = (total - near.astype(jnp.float32))[:FINE].astype(jnp.bfloat16)

    combine(1)

    def stage(step, carry):
        combine(step)
        send_block(pieces, out_ref, sems.at[2], sems.at[3], step - 1, node, spot, core)
        return carry

    lax.fori_loop(2, CHIPS, stage, 0)
    combine(0)
    send_block(pieces, out_ref, sems.at[2], sems.at[3], CHIPS - 1, node, spot, core)

    def send_rest(step, carry):
        send_block(rests, rest_ref, sems.at[4], sems.at[5], step, node, spot, core)
        return carry

    lax.fori_loop(1, CHIPS, send_rest, 0)
    block_of(out_ref, node, spot)[...] = pieces[me]
    block_of(rest_ref, node, spot, FINE)[...] = rests[me]
    whole_wait(rests, sems.at[4], sems.at[5], node, spot, core, "recv")
    whole_wait(rests, sems.at[4], sems.at[5], node, spot, core, "send")
    whole_wait(landing, sems.at[0], sems.at[1], node, spot, core, "send")
    whole_wait(landing, sems.at[2], sems.at[3], node, spot, core, "recv")
    whole_wait(landing, sems.at[2], sems.at[3], node, spot, core, "send")


def weights_kernel(
    weights_ref, new_ref, owner_ref, out_ref, landing, pieces, sems
):
    node, spot, core = position()
    me = node * PLANE + spot
    greet_all(node, spot, core)
    spread(weights_ref, landing, sems.at[0], sems.at[1], node, spot, core)
    whole_wait(landing, sems.at[0], sems.at[1], node, spot, core, "recv")

    def choose(step):
        to_node, to_spot = partner(step, node, spot)
        chip = to_node * PLANE + to_spot
        pieces[chip] = landing[owner_ref[new_ref[chip]]]

    choose(1)

    def stage(step, carry):
        choose(step)
        send_block(pieces, out_ref, sems.at[2], sems.at[3], step - 1, node, spot, core)
        return carry

    lax.fori_loop(2, CHIPS, stage, 0)
    choose(0)
    send_block(pieces, out_ref, sems.at[2], sems.at[3], CHIPS - 1, node, spot, core)
    block_of(out_ref, node, spot)[...] = pieces[me]
    whole_wait(landing, sems.at[0], sems.at[1], node, spot, core, "send")
    whole_wait(landing, sems.at[2], sems.at[3], node, spot, core, "recv")
    whole_wait(landing, sems.at[2], sems.at[3], node, spot, core, "send")


def vmem():
    return pl.BlockSpec(memory_space=pltpu.VMEM)


def smem():
    return pl.BlockSpec(memory_space=pltpu.SMEM)


def combined_grads(slot_grads, slot_tokens, old_slots, owner_chip):
    blocks = (CHIPS, ROWS, COLS)
    half = D // 2
    return pl.pallas_call(
        grads_kernel,
        out_shape=(
            jax.ShapeDtypeStruct((FF, half), jnp.bfloat16),
            jax.ShapeDtypeStruct((PLANE * FINE, half), jnp.bfloat16),
        ),
        in_specs=[pl.BlockSpec(memory_space=pl.ANY), vmem(), vmem(), vmem()],
        out_specs=(vmem(), vmem()),
        scratch_shapes=[
            pltpu.VMEM((FF, half), jnp.bfloat16),
            pltpu.VMEM(blocks, jnp.bfloat16),
            pltpu.VMEM(blocks, jnp.bfloat16),
            pltpu.VMEM((CHIPS, FINE, COLS), jnp.bfloat16),
            pltpu.VMEM((8, CHIPS), jnp.int32),
            pltpu.VMEM((8, CHIPS), jnp.float32),
            pltpu.SMEM((8, CHIPS), jnp.int32),
            pltpu.SMEM((8, CHIPS), jnp.float32),
            pltpu.SemaphoreType.DMA((3,)),
            pltpu.SemaphoreType.DMA((6,)),
        ],
        compiler_params=pltpu.CompilerParams(collective_id=0, has_side_effects=True),
    )(
        slot_grads,
        slot_tokens.reshape(1, CHIPS),
        old_slots.reshape(1, CHIPS),
        owner_chip.reshape(1, CHIPS),
    )


def slot_weights(weights, new_slots, owner_chip):
    blocks = (CHIPS, ROWS, COLS)
    half = D // 2
    return pl.pallas_call(
        weights_kernel,
        out_shape=jax.ShapeDtypeStruct((FF, half), jnp.bfloat16),
        in_specs=[vmem(), smem(), smem()],
        out_specs=vmem(),
        scratch_shapes=[
            pltpu.VMEM(blocks, jnp.bfloat16),
            pltpu.VMEM(blocks, jnp.bfloat16),
            pltpu.SemaphoreType.DMA((4,)),
        ],
        compiler_params=pltpu.CompilerParams(collective_id=1, has_side_effects=True),
    )(weights, new_slots, owner_chip)


def mul(left, right):
    return jnp.dot(
        left.astype(jnp.bfloat16),
        right.astype(jnp.bfloat16),
        preferred_element_type=jnp.float32,
    )


def on_device(slot_grads, slot_tokens, old_slots, owner_chip, momentum, master, new_slots):
    near, rest = combined_grads(slot_grads, slot_tokens, old_slots, owner_chip)
    rest = rest.astype(jnp.float32).reshape(PLANE, FINE, -1)
    rest = jnp.pad(rest, ((0, 0), (0, ROWS - FINE), (0, 0))).reshape(near.shape)
    grad = near.astype(jnp.float32) + rest
    moment = momentum_beta * momentum[0].astype(jnp.float32) + grad
    nesterov = grad + momentum_beta * moment
    part = mul(nesterov, nesterov.T).astype(jnp.bfloat16)
    other = lax.ppermute(part, "column", [(0, 1), (1, 0)])
    gram = part.astype(jnp.float32) + other.astype(jnp.float32)
    scale = 1.0 / (jnp.sqrt(jnp.trace(gram)) + epsilon)
    gram = gram * (scale * scale)
    first = coef_b * gram + coef_c * mul(gram, gram)
    half_way = coef_a * gram + mul(first, gram)
    gram_1 = coef_a * half_way + mul(half_way, first)
    second = coef_b * gram_1 + coef_c * mul(gram_1, gram_1)
    both = coef_a * (first + second) + mul(second, first)
    iterate = (nesterov * (coef_a * coef_a) + mul(both, nesterov)) * scale
    step_scale = learn_rate * 0.2 * math.sqrt(max(FF, D))
    master_new = (1.0 - learn_rate * weight_decay) * master[0] - step_scale * iterate
    slots = slot_weights(master_new.astype(jnp.bfloat16), new_slots, owner_chip)
    return moment.astype(jnp.bfloat16)[None], master_new[None], slots[None]


def solution(mesh):
    split = P(("node", "expert"), None, "column")
    return jax.shard_map(
        on_device,
        mesh=mesh,
        in_specs=(split, P(), P(), P(), split, split, P()),
        out_specs=(split, split, split),
        check_vma=False,
    )
```

```python
import math

import jax
import jax.numpy as jnp
from jax import lax
from jax.experimental import pallas as pl
from jax.experimental.pallas import tpu as pltpu
from jax.sharding import PartitionSpec as P

D = 2048
FF = 768
HALF = D // 2
CHIPS = 128
EXPERTS = 80
NODES = 8
PLANE = 16
ROWS = FF // PLANE
COLS = HALF // NODES
FINE = 16
PARTS = ((FINE, ROWS - FINE), (0, FINE))
TALL = 256
WIDE = 256

coef_a = 3.4445
coef_b = -4.775
coef_c = 2.0315
momentum_beta = 0.95
learn_rate = 1.0
weight_decay = 0.1
epsilon = 1e-07
step_scale = learn_rate * 0.2 * math.sqrt(max(FF, D))

MESH = pl.DeviceIdType.MESH


def partner(step, node, spot):
    to_node = lax.rem(node + lax.rem(step, 8), 8)
    to_x = lax.rem(spot // 4 + lax.rem(step // 8, 4), 4)
    to_y = lax.rem(lax.rem(spot, 4) + step // 32, 4)
    return to_node, to_x * 4 + to_y


def part_of(ref, node, spot, part):
    first, height = PARTS[part]
    rows = pl.ds(pl.multiple_of(spot * ROWS + first, FINE), height)
    cols = pl.ds(pl.multiple_of(node * COLS, COLS), COLS)
    return ref.at[rows, cols]


def rest_of(ref, node, spot):
    rows = pl.ds(pl.multiple_of(spot * FINE, FINE), FINE)
    cols = pl.ds(pl.multiple_of(node * COLS, COLS), COLS)
    return ref.at[rows, cols]


def mul(left, right):
    return jnp.dot(left, right, preferred_element_type=jnp.float32)


def tables(tokens_ref, old_ref, owner_ref, index_ref, weight_ref):
    shape = (CHIPS, CHIPS)
    across = lax.broadcasted_iota(jnp.int32, shape, 1)
    down = lax.broadcasted_iota(jnp.int32, shape, 0)
    owner = jnp.broadcast_to(owner_ref[...], shape).T
    match = (owner == across) & (down < EXPERTS)
    owned = jnp.sum(jnp.where(match, down + 1, 0), axis=0, keepdims=True) - 1
    old = jnp.broadcast_to(old_ref[...], shape).T
    tokens = jnp.broadcast_to(tokens_ref[...], shape).T
    picked = old == owned
    total = jnp.sum(jnp.where(picked, tokens, 0), axis=0, keepdims=True)
    total = jnp.maximum(total.astype(jnp.float32), 1.0)
    for k in range(4):
        first = jnp.min(jnp.where(picked, down, CHIPS), axis=0, keepdims=True)
        here = down == first
        count = jnp.sum(jnp.where(here, tokens, 0), axis=0, keepdims=True)
        weight_ref[k : k + 1, :] = count.astype(jnp.float32) / total
        index_ref[k : k + 1, :] = jnp.where(first < CHIPS, first, 0)
        picked = picked & jnp.logical_not(here)


def step_kernel(
    grads_ref, tokens_ref, old_ref, owner_ref, momentum_ref, master_ref, new_s, owner_s,
    moment_out, master_out, slots_out,
    local, momentum, master, landing_0, landing_1, pieces_0, pieces_1, rests,
    near, rest, x_bf, part, other, gram, gram_bf, first, first_bf, both_bf, change,
    weights, arrived_0, arrived_1, chosen_0, chosen_1,
    index_v, weight_v, index_s, weight_s, copy_sems, sems,
):
    node, spot, core = (lax.axis_index(a) for a in ("node", "expert", "column"))
    me = node * PLANE + spot
    landing, pieces = (landing_0, landing_1), (pieces_0, pieces_1)
    arrived, chosen = (arrived_0, arrived_1), (chosen_0, chosen_1)

    def remote(src, dst, lane, to_node, to_spot, to_core):
        return pltpu.make_async_remote_copy(
            src, dst, sems.at[2 * lane], sems.at[2 * lane + 1],
            device_id=(to_node, to_spot, to_core), device_id_type=MESH,
        )

    def every(body):
        def wrapped(step, carry):
            body(step, *partner(step, node, spot))
            return carry

        lax.fori_loop(1, CHIPS, wrapped, 0)

    def all_of(buffer, lane):
        rows = buffer.at[pl.ds(0, CHIPS - 1)]
        return remote(rows, rows, lane, node, spot, core)

    def spread(source, targets, k, lane):
        def send(step, to_node, to_spot):
            block = part_of(source, to_node, to_spot, k)
            remote(block, targets.at[me], lane, to_node, to_spot, core).start()

        every(send)
        targets[me] = part_of(source, node, spot, k)[...]

    def deliver(make, sources, place, lane):
        def send(step):
            to_node, to_spot = partner(step, node, spot)
            src = sources.at[to_node * PLANE + to_spot]
            remote(src, place, lane, to_node, to_spot, core).start()

        def stage(step, carry):
            make(step)
            send(step - 1)
            return carry

        make(1)
        lax.fori_loop(2, CHIPS, stage, 0)
        make(0)
        send(CHIPS - 1)
        place[...] = sources[me]

    loads = (
        pltpu.make_async_copy(grads_ref.at[0], local, copy_sems.at[0]),
        pltpu.make_async_copy(momentum_ref.at[0], momentum, copy_sems.at[1]),
        pltpu.make_async_copy(master_ref.at[0], master, copy_sems.at[2]),
    )
    for load in loads:
        load.start()

    barrier = pltpu.get_barrier_semaphore()

    def greet(step, to_node, to_spot):
        pl.semaphore_signal(
            barrier, inc=1, device_id=(to_node, to_spot, core), device_id_type=MESH
        )

    every(greet)
    pl.semaphore_signal(barrier, inc=1, device_id=(node, spot, 1 - core), device_id_type=MESH)
    pl.semaphore_wait(barrier, CHIPS)
    loads[0].wait()
    for k in range(2):
        spread(local, landing[k], k, k)

    tables(tokens_ref, old_ref, owner_ref, index_v, weight_v)
    to_smem = (
        pltpu.make_async_copy(index_v, index_s, copy_sems.at[3]),
        pltpu.make_async_copy(weight_v, weight_s, copy_sems.at[4]),
    )
    for copy in to_smem:
        copy.start()
    for copy in to_smem:
        copy.wait()

    for k in range(2):
        all_of(landing[k], k).wait_recv()

        def combine(step, k=k):
            to_node, to_spot = partner(step, node, spot)
            chip = to_node * PLANE + to_spot
            total = landing[k][index_s[0, chip]].astype(jnp.float32) * weight_s[0, chip]
            for j in range(1, 4):
                slot = landing[k][index_s[j, chip]].astype(jnp.float32)
                total += slot * weight_s[j, chip]
            rounded = total.astype(jnp.bfloat16)
            pieces[k][chip] = rounded
            if k == 1:
                rests[chip] = (total - rounded.astype(jnp.float32)).astype(jnp.bfloat16)

        deliver(combine, pieces[k], part_of(near, node, spot, k), 2 + k)

    def send_rest(step, to_node, to_spot):
        src = rests.at[to_node * PLANE + to_spot]
        remote(src, rest_of(rest, node, spot), 4, to_node, to_spot, core).start()

    every(send_rest)
    rest_of(rest, node, spot)[...] = rests[me]

    def rows_of(block, k):
        start, height = PARTS[k]
        return pl.ds(pl.multiple_of(block * ROWS + start, FINE), height)

    loads[1].wait()
    for k in range(2):
        all_of(pieces[k], 2 + k).wait_recv()

        def direction(block, carry, k=k):
            rows = rows_of(block, k)
            grad = near[rows, :].astype(jnp.float32)
            moment = momentum_beta * momentum[rows, :].astype(jnp.float32) + grad
            x_bf[rows, :] = (grad + momentum_beta * moment).astype(jnp.bfloat16)
            return carry

        lax.fori_loop(0, PLANE, direction, 0)

    def band(i):
        return pl.ds(pl.multiple_of(i * TALL, TALL), TALL)

    bands = FF // TALL

    def gram_band(i, carry):
        product = lax.dot_general(
            x_bf[band(i), :], x_bf[...], (((1,), (1,)), ((), ())),
            preferred_element_type=jnp.float32,
        )
        part[band(i), :] = product.astype(jnp.bfloat16)
        return carry

    lax.fori_loop(0, bands, gram_band, 0)
    swap = remote(part, other, 5, node, spot, 1 - core)

    def own_band(i, carry):
        gram[band(i), :] = part[band(i), :].astype(jnp.float32)
        return carry

    lax.fori_loop(0, bands, own_band, 0)
    swap.start()
    swap.wait_recv()

    eye = (CHIPS, CHIPS)
    on_diagonal = lax.broadcasted_iota(jnp.int32, eye, 0) == lax.broadcasted_iota(
        jnp.int32, eye, 1
    )
    diagonal = jnp.zeros(eye, jnp.float32)
    for i in range(FF // CHIPS):
        at = slice(i * CHIPS, (i + 1) * CHIPS)
        diagonal += jnp.where(on_diagonal, gram[at, at] + other[at, at].astype(jnp.float32), 0.0)
    squares = jnp.sum(jnp.sum(diagonal, axis=0, keepdims=True), axis=1, keepdims=True)
    scale = 1.0 / (jnp.sqrt(squares) + epsilon)
    scale_2 = scale * scale

    def scale_band(i, carry):
        scaled = (gram[band(i), :] + other[band(i), :].astype(jnp.float32)) * scale_2
        gram[band(i), :] = scaled
        gram_bf[band(i), :] = scaled.astype(jnp.bfloat16)
        return carry

    lax.fori_loop(0, bands, scale_band, 0)

    def first_band(i, carry):
        value = coef_b * gram[band(i), :] + coef_c * mul(gram_bf[band(i), :], gram_bf[...])
        first[band(i), :] = value
        first_bf[band(i), :] = value.astype(jnp.bfloat16)
        return carry

    lax.fori_loop(0, bands, first_band, 0)

    def next_band(i, carry):
        half_way = coef_a * gram[band(i), :] + mul(first_bf[band(i), :], gram_bf[...])
        after = coef_a * half_way + mul(half_way.astype(jnp.bfloat16), first_bf[...])
        gram[band(i), :] = after
        return carry

    lax.fori_loop(0, bands, next_band, 0)

    def round_band(i, carry):
        gram_bf[band(i), :] = gram[band(i), :].astype(jnp.bfloat16)
        return carry

    lax.fori_loop(0, bands, round_band, 0)

    def both_band(i, carry):
        second = coef_b * gram[band(i), :] + coef_c * mul(gram_bf[band(i), :], gram_bf[...])
        value = coef_a * (first[band(i), :] + second)
        value += mul(second.astype(jnp.bfloat16), first_bf[...])
        both_bf[band(i), :] = value.astype(jnp.bfloat16)
        return carry

    lax.fori_loop(0, bands, both_band, 0)

    def change_band(i, carry):
        cols = pl.ds(pl.multiple_of(i * WIDE, WIDE), WIDE)
        change[:, cols] = mul(both_bf[...], x_bf[:, cols])
        return carry

    lax.fori_loop(0, HALF // WIDE, change_band, 0)

    loads[2].wait()
    length = step_scale * scale
    for k in range(2):
        if k == 1:
            all_of(rests, 4).wait_recv()

        def update(block, carry, k=k):
            rows = rows_of(block, k)
            grad = near[rows, :].astype(jnp.float32)
            if k == 1:
                fine_rows = pl.ds(pl.multiple_of(block * FINE, FINE), FINE)
                grad += rest[fine_rows, :].astype(jnp.float32)
            moment = momentum_beta * momentum[rows, :].astype(jnp.float32) + grad
            moment_out[rows, :] = moment.astype(jnp.bfloat16)
            iterate = (coef_a * coef_a) * (grad + momentum_beta * moment) + change[rows, :]
            value = (1.0 - learn_rate * weight_decay) * master[rows, :] - length * iterate
            master_out[rows, :] = value
            weights[rows, :] = value.astype(jnp.bfloat16)
            return carry

        lax.fori_loop(0, PLANE, update, 0)
        spread(weights, arrived[k], k, 6 + k)

    for k in range(2):
        all_of(arrived[k], 6 + k).wait_recv()

        def choose(step, k=k):
            to_node, to_spot = partner(step, node, spot)
            chip = to_node * PLANE + to_spot
            chosen[k][chip] = arrived[k][owner_s[new_s[chip]]]

        deliver(choose, chosen[k], part_of(slots_out, node, spot, k), 8 + k)

    for k in range(2):
        all_of(chosen[k], 8 + k).wait_recv()
        for lane in (0, 2, 6, 8):
            all_of(chosen[k], lane + k).wait_send()
    all_of(rests, 4).wait_send()
    swap.wait_send()


def write_kernel(moment_ref, master_ref, slots_ref, moment_out, master_out, slots_out, sems):
    copies = [
        pltpu.make_async_copy(source, target.at[0], sems.at[i])
        for i, (source, target) in enumerate(
            ((master_ref, master_out), (moment_ref, moment_out), (slots_ref, slots_out))
        )
    ]
    for copy in copies:
        copy.start()
    for copy in copies:
        copy.wait()


def on_device(slot_grads, slot_tokens, old_slots, owner_chip, momentum, master, new_slots):
    bf, f32 = jnp.bfloat16, jnp.float32
    vmem = pl.BlockSpec(memory_space=pltpu.VMEM)
    smem = pl.BlockSpec(memory_space=pltpu.SMEM)
    hbm = pl.BlockSpec(memory_space=pl.ANY)
    matrix = (FF, HALF)
    square = (FF, FF)
    tall = (CHIPS, PARTS[0][1], COLS)
    low = (CHIPS, FINE, COLS)
    row = (1, CHIPS)
    kept = (pltpu.VMEM(matrix, bf), pltpu.VMEM(matrix, f32), pltpu.VMEM(matrix, bf))
    moment_new, master_new, slots = pl.pallas_call(
        step_kernel,
        out_shape=kept,
        in_specs=[hbm, vmem, vmem, vmem, hbm, hbm, smem, smem],
        out_specs=(vmem, vmem, vmem),
        scratch_shapes=[
            pltpu.VMEM(matrix, bf),
            pltpu.VMEM(matrix, bf),
            pltpu.VMEM(matrix, f32),
            pltpu.VMEM(tall, bf),
            pltpu.VMEM(low, bf),
            pltpu.VMEM(tall, bf),
            pltpu.VMEM(low, bf),
            pltpu.VMEM(low, bf),
            pltpu.VMEM(matrix, bf),
            pltpu.VMEM((PLANE * FINE, HALF), bf),
            pltpu.VMEM(matrix, bf),
            pltpu.VMEM(square, bf),
            pltpu.VMEM(square, bf),
            pltpu.VMEM(square, f32),
            pltpu.VMEM(square, bf),
            pltpu.VMEM(square, f32),
            pltpu.VMEM(square, bf),
            pltpu.VMEM(square, bf),
            pltpu.VMEM(matrix, f32),
            pltpu.VMEM(matrix, bf),
            pltpu.VMEM(tall, bf),
            pltpu.VMEM(low, bf),
            pltpu.VMEM(tall, bf),
            pltpu.VMEM(low, bf),
            pltpu.VMEM((8, CHIPS), jnp.int32),
            pltpu.VMEM((8, CHIPS), f32),
            pltpu.SMEM((8, CHIPS), jnp.int32),
            pltpu.SMEM((8, CHIPS), f32),
            pltpu.SemaphoreType.DMA((5,)),
            pltpu.SemaphoreType.DMA((20,)),
        ],
        compiler_params=pltpu.CompilerParams(
            collective_id=0, has_side_effects=True, vmem_limit_bytes=50 * 2**20
        ),
    )(
        slot_grads,
        slot_tokens.reshape(row),
        old_slots.reshape(row),
        owner_chip.reshape(row),
        momentum,
        master,
        new_slots,
        owner_chip,
    )
    outs = tuple(jax.ShapeDtypeStruct((1, *matrix), kind) for kind in (bf, f32, bf))
    return pl.pallas_call(
        write_kernel,
        out_shape=outs,
        in_specs=[vmem, vmem, vmem],
        out_specs=(hbm, hbm, hbm),
        scratch_shapes=[pltpu.SemaphoreType.DMA((3,))],
        compiler_params=pltpu.CompilerParams(vmem_limit_bytes=2**20),
    )(moment_new, master_new, slots)


def solution(mesh):
    split = P(("node", "expert"), None, "column")
    return jax.shard_map(
        on_device,
        mesh=mesh,
        in_specs=(split, P(), P(), P(), split, split, P()),
        out_specs=(split, split, split),
        check_vma=False,
    )
```

```python
import math

import jax
import jax.numpy as jnp
from jax import lax
from jax.experimental import pallas as pl
from jax.experimental.pallas import tpu as pltpu
from jax.sharding import PartitionSpec as P

D = 2048
FF = 768
HALF = D // 2
CHIPS = 128
EXPERTS = 80
NODES = 8
PLANE = 16
ROWS = FF // PLANE
COLS = HALF // NODES
FINE = 16
PARTS = ((FINE, ROWS - FINE), (0, FINE))
WIDE = 256

coef_a = 3.4445
coef_b = -4.775
coef_c = 2.0315
momentum_beta = 0.95
learn_rate = 1.0
weight_decay = 0.1
epsilon = 1e-07
code_scale = 2.0**27
step_scale = learn_rate * 0.2 * math.sqrt(max(FF, D))

MESH = pl.DeviceIdType.MESH


def partner(step, node, spot):
    to_node = lax.rem(node + lax.rem(step, 8), 8)
    to_x = lax.rem(spot // 4 + lax.rem(step // 8, 4), 4)
    to_y = lax.rem(lax.rem(spot, 4) + step // 32, 4)
    return to_node, to_x * 4 + to_y


def part_of(ref, node, spot, part):
    first, height = PARTS[part]
    rows = pl.ds(pl.multiple_of(spot * ROWS + first, FINE), height)
    cols = pl.ds(pl.multiple_of(node * COLS, COLS), COLS)
    return ref.at[rows, cols]


def coded(grad):
    large = grad * code_scale
    return ((large * large) * (large * jnp.abs(large))).astype(jnp.bfloat16)


def decoded(code):
    code = code.astype(jnp.float32)
    size = lax.rsqrt(lax.rsqrt(jnp.abs(code))) * (1.0 / code_scale)
    size = jnp.where(code == 0.0, 0.0, size)
    return jnp.where(code < 0.0, -size, size)


def mul(left, right):
    return jnp.dot(left, right, preferred_element_type=jnp.float32)


def tables(tokens_ref, old_ref, owner_ref, index_ref, weight_ref):
    shape = (CHIPS, CHIPS)
    across = lax.broadcasted_iota(jnp.int32, shape, 1)
    down = lax.broadcasted_iota(jnp.int32, shape, 0)
    owner = jnp.broadcast_to(owner_ref[...], shape).T
    match = (owner == across) & (down < EXPERTS)
    owned = jnp.sum(jnp.where(match, down + 1, 0), axis=0, keepdims=True) - 1
    old = jnp.broadcast_to(old_ref[...], shape).T
    tokens = jnp.broadcast_to(tokens_ref[...], shape).T
    picked = old == owned
    total = jnp.sum(jnp.where(picked, tokens, 0), axis=0, keepdims=True)
    total = jnp.maximum(total.astype(jnp.float32), 1.0)
    for k in range(4):
        first = jnp.min(jnp.where(picked, down, CHIPS), axis=0, keepdims=True)
        here = down == first
        count = jnp.sum(jnp.where(here, tokens, 0), axis=0, keepdims=True)
        weight_ref[k : k + 1, :] = count.astype(jnp.float32) / total
        index_ref[k : k + 1, :] = jnp.where(first < CHIPS, first, 0)
        picked = picked & jnp.logical_not(here)


def step_kernel(
    grads_ref, tokens_ref, old_ref, owner_ref, momentum_ref, master_ref, new_s, owner_s,
    moment_out, master_out, slots_out,
    local, momentum, master, landing_0, landing_1, pieces_0, pieces_1,
    near, nesterov, x_bf, part, other, gram, gram_bf, first, first_bf, next_bf, both_bf, change,
    weights, arrived_0, arrived_1, chosen_0, chosen_1,
    index_v, weight_v, index_s, weight_s, copy_sems, sems,
):
    node, spot, core = (lax.axis_index(a) for a in ("node", "expert", "column"))
    me = node * PLANE + spot
    landing, pieces = (landing_0, landing_1), (pieces_0, pieces_1)
    arrived, chosen = (arrived_0, arrived_1), (chosen_0, chosen_1)

    def remote(src, dst, lane, to_node, to_spot, to_core):
        return pltpu.make_async_remote_copy(
            src, dst, sems.at[2 * lane], sems.at[2 * lane + 1],
            device_id=(to_node, to_spot, to_core), device_id_type=MESH,
        )

    near_nodes = [lax.rem(node + by_node, NODES) for by_node in range(NODES)]

    def spot_at(step):
        to_x = lax.rem(spot // 4 + step // 4, 4)
        return to_x * 4 + lax.rem(lax.rem(spot, 4) + lax.rem(step, 4), 4)

    def every(body):
        for to_node in near_nodes[1:]:
            body(to_node, spot)

        def wrapped(step, carry):
            to_spot = spot_at(step)
            for to_node in near_nodes:
                body(to_node, to_spot)
            return carry

        lax.fori_loop(1, PLANE, wrapped, 0)

    def all_of(buffer, lane):
        rows = buffer.at[pl.ds(0, CHIPS - 1)]
        return remote(rows, rows, lane, node, spot, core)

    def spread(source, targets, k, lane):
        def send(to_node, to_spot):
            block = part_of(source, to_node, to_spot, k)
            remote(block, targets.at[me], lane, to_node, to_spot, core).start()

        every(send)
        targets[me] = part_of(source, node, spot, k)[...]

    def deliver(make, sources, place, lane):
        def send(step):
            to_node, to_spot = partner(step, node, spot)
            src = sources.at[to_node * PLANE + to_spot]
            remote(src, place, lane, to_node, to_spot, core).start()

        def stage(step, carry):
            make(step)
            send(step - 1)
            return carry

        make(1)
        lax.fori_loop(2, CHIPS, stage, 0)
        make(0)
        send(CHIPS - 1)
        place[...] = sources[me]

    loads = (
        pltpu.make_async_copy(grads_ref.at[0], local, copy_sems.at[0]),
        pltpu.make_async_copy(momentum_ref.at[0], momentum, copy_sems.at[1]),
        pltpu.make_async_copy(master_ref.at[0], master, copy_sems.at[2]),
    )
    for load in loads:
        load.start()

    barrier = pltpu.get_barrier_semaphore()

    def greet(to_node, to_spot):
        pl.semaphore_signal(
            barrier, inc=1, device_id=(to_node, to_spot, core), device_id_type=MESH
        )

    every(greet)
    pl.semaphore_signal(barrier, inc=1, device_id=(node, spot, 1 - core), device_id_type=MESH)
    pl.semaphore_wait(barrier, CHIPS)
    loads[0].wait()
    for k in range(2):
        spread(local, landing[k], k, k)

    tables(tokens_ref, old_ref, owner_ref, index_v, weight_v)
    to_smem = (
        pltpu.make_async_copy(index_v, index_s, copy_sems.at[3]),
        pltpu.make_async_copy(weight_v, weight_s, copy_sems.at[4]),
    )
    for copy in to_smem:
        copy.start()
    for copy in to_smem:
        copy.wait()

    parity = lax.rem(node + spot // 4 + lax.rem(spot, 4), 2)

    def combine(chip, k):
        total = landing[k][index_s[0, chip]].astype(jnp.float32) * weight_s[0, chip]
        for j in range(1, 4):
            slot = landing[k][index_s[j, chip]].astype(jnp.float32)
            total += slot * weight_s[j, chip]
        pieces[k][chip] = coded(total)

    def combine_half(half, k):
        offset = lax.rem(parity + half, 2)
        place = part_of(near, node, spot, k)

        def chips_at(step):
            odd = lax.rem(offset + step // 4 + lax.rem(step, 4), 2)
            nodes = [lax.rem(node + odd + by_node, NODES) for by_node in range(0, NODES, 2)]
            return nodes, spot_at(step)

        def make(step):
            nodes, to_spot = chips_at(step)
            for to_node in nodes:
                combine(to_node * PLANE + to_spot, k)

        def send(step, skip_own=False):
            nodes, to_spot = chips_at(step)
            for i, to_node in enumerate(nodes):
                src = pieces[k].at[to_node * PLANE + to_spot]
                copy = remote(src, place, 2 + k, to_node, to_spot, core)
                if skip_own and i == 0:
                    pl.when(offset == 1)(copy.start)
                else:
                    copy.start()

        def stage(step, carry):
            make(step)
            send(step - 1)
            return carry

        make(0)
        make(1)
        send(0, skip_own=True)
        lax.fori_loop(2, PLANE, stage, 0)
        if half == 1:
            combine(me, k)
            place[...] = pieces[k][me]
        send(PLANE - 1)

    for half in range(2):
        for k in range(2):
            if half == 0:
                all_of(landing[k], k).wait_recv()
            combine_half(half, k)

    def rows_of(block, k):
        start, height = PARTS[k]
        return pl.ds(pl.multiple_of(block * ROWS + start, FINE), height)

    loads[1].wait()
    for k in range(2):
        all_of(pieces[k], 2 + k).wait_recv()

        def direction(block, carry, k=k):
            rows = rows_of(block, k)
            grad = decoded(near[rows, :])
            moment = momentum_beta * momentum[rows, :].astype(jnp.float32) + grad
            moment_out[rows, :] = moment.astype(jnp.bfloat16)
            ahead = grad + momentum_beta * moment
            nesterov[rows, :] = ahead
            x_bf[rows, :] = ahead.astype(jnp.bfloat16)
            return carry

        lax.fori_loop(0, PLANE, direction, 0, unroll=2)

    bands = [pl.ds(i * WIDE, WIDE) for i in range(FF // WIDE)]

    def swap_band(i):
        at = (slice(None), bands[i])
        return remote(part.at[at], other.at[at], 5, node, spot, 1 - core)

    for i, cols in enumerate(bands):
        product = lax.dot_general(
            x_bf[...], x_bf[cols, :], (((1,), (1,)), ((), ())),
            preferred_element_type=jnp.float32,
        )
        part[:, cols] = product.astype(jnp.bfloat16)
        if i > 0:
            swap_band(i - 1).start()
    eye = (CHIPS, CHIPS)
    on_diagonal = lax.broadcasted_iota(jnp.int32, eye, 0) == lax.broadcasted_iota(
        jnp.int32, eye, 1
    )

    def diagonal_of(ref):
        total = jnp.zeros(eye, jnp.float32)
        for i in range(FF // CHIPS):
            at = slice(i * CHIPS, (i + 1) * CHIPS)
            total += jnp.where(on_diagonal, ref[at, at].astype(jnp.float32), 0.0)
        return total

    diagonal = diagonal_of(part)
    swap_band(len(bands) - 1).start()
    remote(part, other, 5, node, spot, 1 - core).wait_recv()
    diagonal += diagonal_of(other)
    squares = jnp.sum(jnp.sum(diagonal, axis=0, keepdims=True), axis=1, keepdims=True)
    scale = 1.0 / (jnp.sqrt(squares) + epsilon)
    scale_2 = scale * scale
    for cols in bands:
        both = part[:, cols].astype(jnp.float32) + other[:, cols].astype(jnp.float32)
        scaled = both * scale_2
        gram[:, cols] = scaled
        gram_bf[:, cols] = scaled.astype(jnp.bfloat16)

    for cols in bands:
        value = coef_b * gram[:, cols] + coef_c * mul(gram_bf[...], gram_bf[:, cols])
        first[:, cols] = value
        first_bf[:, cols] = value.astype(jnp.bfloat16)
    for cols in bands:
        half_way = coef_a * gram[:, cols] + mul(first_bf[...], gram_bf[:, cols])
        after = coef_a * half_way + mul(first_bf[...], half_way.astype(jnp.bfloat16))
        gram[:, cols] = after
        next_bf[:, cols] = after.astype(jnp.bfloat16)
    for cols in bands:
        second = coef_b * gram[:, cols] + coef_c * mul(next_bf[...], next_bf[:, cols])
        value = coef_a * (first[:, cols] + second)
        value += mul(first_bf[...], second.astype(jnp.bfloat16))
        both_bf[:, cols] = value.astype(jnp.bfloat16)

    loads[2].wait()
    length = step_scale * scale

    pairs = NODES // 2
    for i in range(pairs):
        pair = lax.rem(node // 2 + i, pairs)
        cols = pl.ds(pl.multiple_of(pair * WIDE, WIDE), WIDE)
        change[:, cols] = mul(both_bf[...], x_bf[:, cols])

        def update(block, carry, cols=cols):
            rows = pl.ds(pl.multiple_of(block * ROWS, ROWS), ROWS)
            iterate = (coef_a * coef_a) * nesterov[rows, cols] + change[rows, cols]
            value = (1.0 - learn_rate * weight_decay) * master[rows, cols] - length * iterate
            master_out[rows, cols] = value
            weights[rows, cols] = value.astype(jnp.bfloat16)
            return carry

        lax.fori_loop(0, PLANE, update, 0, unroll=4)

        def send_weights(step, carry, pair=pair):
            to_node = 2 * pair + lax.rem(node + step, 2)
            to_x = lax.rem(spot // 4 + lax.rem(step // 2, 4), 4)
            to_y = lax.rem(lax.rem(spot, 4) + step // 8, 4)
            to_spot = to_x * 4 + to_y
            block = part_of(weights, to_node, to_spot, 0)
            remote(block, arrived[0].at[me], 6, to_node, to_spot, core).start()
            return carry

        lax.fori_loop(1 if i == 0 else 0, 2 * PLANE, send_weights, 0)

    spread(weights, arrived[1], 1, 7)
    arrived[0][me] = part_of(weights, node, spot, 0)[...]

    for k in range(2):
        all_of(arrived[k], 6 + k).wait_recv()

        def choose(step, k=k):
            to_node, to_spot = partner(step, node, spot)
            chip = to_node * PLANE + to_spot
            chosen[k][chip] = arrived[k][owner_s[new_s[chip]]]

        deliver(choose, chosen[k], part_of(slots_out, node, spot, k), 8 + k)

    for k in range(2):
        all_of(chosen[k], 8 + k).wait_recv()
        for lane in (0, 2, 6, 8):
            all_of(chosen[k], lane + k).wait_send()
    remote(part, other, 5, node, spot, 1 - core).wait_send()


def write_kernel(moment_ref, master_ref, slots_ref, moment_out, master_out, slots_out, sems):
    copies = [
        pltpu.make_async_copy(source, target.at[0], sems.at[i])
        for i, (source, target) in enumerate(
            ((master_ref, master_out), (moment_ref, moment_out), (slots_ref, slots_out))
        )
    ]
    for copy in copies:
        copy.start()
    for copy in copies:
        copy.wait()


def on_device(slot_grads, slot_tokens, old_slots, owner_chip, momentum, master, new_slots):
    bf, f32 = jnp.bfloat16, jnp.float32
    vmem = pl.BlockSpec(memory_space=pltpu.VMEM)
    smem = pl.BlockSpec(memory_space=pltpu.SMEM)
    hbm = pl.BlockSpec(memory_space=pl.ANY)
    matrix = (FF, HALF)
    square = (FF, FF)
    tall = (CHIPS, PARTS[0][1], COLS)
    low = (CHIPS, FINE, COLS)
    row = (1, CHIPS)
    kept = (pltpu.VMEM(matrix, bf), pltpu.VMEM(matrix, f32), pltpu.VMEM(matrix, bf))
    moment_new, master_new, slots = pl.pallas_call(
        step_kernel,
        out_shape=kept,
        in_specs=[hbm, vmem, vmem, vmem, hbm, hbm, smem, smem],
        out_specs=(vmem, vmem, vmem),
        scratch_shapes=[
            pltpu.VMEM(matrix, bf),
            pltpu.VMEM(matrix, bf),
            pltpu.VMEM(matrix, f32),
            pltpu.VMEM(tall, bf),
            pltpu.VMEM(low, bf),
            pltpu.VMEM(tall, bf),
            pltpu.VMEM(low, bf),
            pltpu.VMEM(matrix, bf),
            pltpu.VMEM(matrix, f32),
            pltpu.VMEM(matrix, bf),
            pltpu.VMEM(square, bf),
            pltpu.VMEM(square, bf),
            pltpu.VMEM(square, f32),
            pltpu.VMEM(square, bf),
            pltpu.VMEM(square, f32),
            pltpu.VMEM(square, bf),
            pltpu.VMEM(square, bf),
            pltpu.VMEM(square, bf),
            pltpu.VMEM(matrix, f32),
            pltpu.VMEM(matrix, bf),
            pltpu.VMEM(tall, bf),
            pltpu.VMEM(low, bf),
            pltpu.VMEM(tall, bf),
            pltpu.VMEM(low, bf),
            pltpu.VMEM((8, CHIPS), jnp.int32),
            pltpu.VMEM((8, CHIPS), f32),
            pltpu.SMEM((8, CHIPS), jnp.int32),
            pltpu.SMEM((8, CHIPS), f32),
            pltpu.SemaphoreType.DMA((5,)),
            pltpu.SemaphoreType.DMA((20,)),
        ],
        compiler_params=pltpu.CompilerParams(
            collective_id=0, has_side_effects=True, vmem_limit_bytes=50 * 2**20
        ),
    )(
        slot_grads,
        slot_tokens.reshape(row),
        old_slots.reshape(row),
        owner_chip.reshape(row),
        momentum,
        master,
        new_slots,
        owner_chip,
    )
    outs = tuple(jax.ShapeDtypeStruct((1, *matrix), kind) for kind in (bf, f32, bf))
    return pl.pallas_call(
        write_kernel,
        out_shape=outs,
        in_specs=[vmem, vmem, vmem],
        out_specs=(hbm, hbm, hbm),
        scratch_shapes=[pltpu.SemaphoreType.DMA((3,))],
        compiler_params=pltpu.CompilerParams(vmem_limit_bytes=2**20),
    )(moment_new, master_new, slots)


def solution(mesh):
    split = P(("node", "expert"), None, "column")
    return jax.shard_map(
        on_device,
        mesh=mesh,
        in_specs=(split, P(), P(), P(), split, split, P()),
        out_specs=(split, split, split),
        check_vma=False,
    )
```

```python
import math

import jax
import jax.numpy as jnp
from jax import lax
from jax.experimental import pallas as pl
from jax.experimental.pallas import tpu as pltpu
from jax.sharding import PartitionSpec as P

D = 2048
FF = 768
HALF = D // 2
CHIPS = 128
EXPERTS = 80
NODES = 8
PLANE = 16
ROWS = FF // PLANE
COLS = HALF // NODES
FINE = 16
PARTS = ((FINE, ROWS - FINE), (0, FINE))
WIDE = 256
EARLY = PLANE * PARTS[0][1]

coef_a = 3.4445
coef_b = -4.775
coef_c = 2.0315
momentum_beta = 0.95
learn_rate = 1.0
weight_decay = 0.1
epsilon = 1e-07
code_scale = 2.0**27
step_scale = learn_rate * 0.2 * math.sqrt(max(FF, D))

MESH = pl.DeviceIdType.MESH


def partner(step, node, spot):
    to_node = lax.rem(node + lax.rem(step, 8), 8)
    to_x = lax.rem(spot // 4 + lax.rem(step // 8, 4), 4)
    to_y = lax.rem(lax.rem(spot, 4) + step // 32, 4)
    return to_node, to_x * 4 + to_y


def part_of(ref, node, spot, part):
    first, height = PARTS[part]
    rows = pl.ds(pl.multiple_of(spot * ROWS + first, FINE), height)
    cols = pl.ds(pl.multiple_of(node * COLS, COLS), COLS)
    return ref.at[rows, cols]


def coded(grad):
    large = grad * code_scale
    return ((large * large) * (large * jnp.abs(large))).astype(jnp.bfloat16)


def decoded(code):
    code = code.astype(jnp.float32)
    size = lax.rsqrt(lax.rsqrt(jnp.abs(code))) * (1.0 / code_scale)
    size = jnp.where(code == 0.0, 0.0, size)
    return jnp.where(code < 0.0, -size, size)


def mul(left, right):
    return jnp.dot(left, right, preferred_element_type=jnp.float32)


def tables(tokens_ref, old_ref, owner_ref, index_ref, weight_ref):
    shape = (CHIPS, CHIPS)
    across = lax.broadcasted_iota(jnp.int32, shape, 1)
    down = lax.broadcasted_iota(jnp.int32, shape, 0)
    owner = jnp.broadcast_to(owner_ref[...], shape).T
    match = (owner == across) & (down < EXPERTS)
    owned = jnp.sum(jnp.where(match, down + 1, 0), axis=0, keepdims=True) - 1
    old = jnp.broadcast_to(old_ref[...], shape).T
    tokens = jnp.broadcast_to(tokens_ref[...], shape).T
    picked = old == owned
    total = jnp.sum(jnp.where(picked, tokens, 0), axis=0, keepdims=True)
    total = jnp.maximum(total.astype(jnp.float32), 1.0)
    for k in range(4):
        first = jnp.min(jnp.where(picked, down, CHIPS), axis=0, keepdims=True)
        here = down == first
        count = jnp.sum(jnp.where(here, tokens, 0), axis=0, keepdims=True)
        weight_ref[k : k + 1, :] = count.astype(jnp.float32) / total
        index_ref[k : k + 1, :] = jnp.where(first < CHIPS, first, 0)
        picked = picked & jnp.logical_not(here)


def step_kernel(
    grads_ref, tokens_ref, old_ref, owner_ref, momentum_ref, master_ref, new_s, owner_s,
    moment_out, master_out, slots_out,
    local, momentum, master, landing_0, landing_1, pieces_0, pieces_1,
    near, nesterov, x_bf, part, other, gram, gram_bf, first, first_bf, next_bf, both_bf, change,
    weights, arrived_0, arrived_1, chosen_0, chosen_1,
    index_v, weight_v, index_s, weight_s, copy_sems, sems,
):
    node, spot, core = (lax.axis_index(a) for a in ("node", "expert", "column"))
    me = node * PLANE + spot
    landing, pieces = (landing_0, landing_1), (pieces_0, pieces_1)
    arrived, chosen = (arrived_0, arrived_1), (chosen_0, chosen_1)

    def remote(src, dst, lane, to_node, to_spot, to_core):
        return pltpu.make_async_remote_copy(
            src, dst, sems.at[2 * lane], sems.at[2 * lane + 1],
            device_id=(to_node, to_spot, to_core), device_id_type=MESH,
        )

    near_nodes = [lax.rem(node + by_node, NODES) for by_node in range(NODES)]

    def spot_at(step):
        to_x = lax.rem(spot // 4 + step // 4, 4)
        return to_x * 4 + lax.rem(lax.rem(spot, 4) + lax.rem(step, 4), 4)

    def every(body):
        for to_node in near_nodes[1:]:
            body(to_node, spot)

        def wrapped(step, carry):
            to_spot = spot_at(step)
            for to_node in near_nodes:
                body(to_node, to_spot)
            return carry

        lax.fori_loop(1, PLANE, wrapped, 0)

    def all_of(buffer, lane):
        rows = buffer.at[pl.ds(0, CHIPS - 1)]
        return remote(rows, rows, lane, node, spot, core)

    def spread(source, targets, k, lane):
        def send(to_node, to_spot):
            block = part_of(source, to_node, to_spot, k)
            remote(block, targets.at[me], lane, to_node, to_spot, core).start()

        every(send)
        targets[me] = part_of(source, node, spot, k)[...]

    def deliver(make, sources, place, lane):
        def send(step):
            to_node, to_spot = partner(step, node, spot)
            src = sources.at[to_node * PLANE + to_spot]
            remote(src, place, lane, to_node, to_spot, core).start()

        def stage(step, carry):
            make(step)
            send(step - 1)
            return carry

        make(1)
        lax.fori_loop(2, CHIPS, stage, 0)
        make(0)
        send(CHIPS - 1)
        place[...] = sources[me]

    loads = (
        pltpu.make_async_copy(grads_ref.at[0], local, copy_sems.at[0]),
        pltpu.make_async_copy(momentum_ref.at[0], momentum, copy_sems.at[1]),
        pltpu.make_async_copy(master_ref.at[0], master, copy_sems.at[2]),
    )
    for load in loads:
        load.start()

    barrier = pltpu.get_barrier_semaphore()

    def greet(to_node, to_spot):
        pl.semaphore_signal(
            barrier, inc=1, device_id=(to_node, to_spot, core), device_id_type=MESH
        )

    every(greet)
    pl.semaphore_signal(barrier, inc=1, device_id=(node, spot, 1 - core), device_id_type=MESH)
    pl.semaphore_wait(barrier, CHIPS)
    loads[0].wait()
    for k in range(2):
        spread(local, landing[k], k, k)

    tables(tokens_ref, old_ref, owner_ref, index_v, weight_v)
    to_smem = (
        pltpu.make_async_copy(index_v, index_s, copy_sems.at[3]),
        pltpu.make_async_copy(weight_v, weight_s, copy_sems.at[4]),
    )
    for copy in to_smem:
        copy.start()
    for copy in to_smem:
        copy.wait()

    parity = lax.rem(node + spot // 4 + lax.rem(spot, 4), 2)

    def combine(chip, k):
        total = landing[k][index_s[0, chip]].astype(jnp.float32) * weight_s[0, chip]
        for j in range(1, 4):
            slot = landing[k][index_s[j, chip]].astype(jnp.float32)
            total += slot * weight_s[j, chip]
        pieces[k][chip] = coded(total)

    def combine_half(half, k):
        offset = lax.rem(parity + half, 2)
        place = part_of(near, node, spot, k)

        def chips_at(step):
            odd = lax.rem(offset + step // 4 + lax.rem(step, 4), 2)
            nodes = [lax.rem(node + odd + by_node, NODES) for by_node in range(0, NODES, 2)]
            return nodes, spot_at(step)

        def make(step):
            nodes, to_spot = chips_at(step)
            for to_node in nodes:
                combine(to_node * PLANE + to_spot, k)

        def send(step, skip_own=False):
            nodes, to_spot = chips_at(step)
            for i, to_node in enumerate(nodes):
                src = pieces[k].at[to_node * PLANE + to_spot]
                copy = remote(src, place, 2 + k, to_node, to_spot, core)
                if skip_own and i == 0:
                    pl.when(offset == 1)(copy.start)
                else:
                    copy.start()

        def stage(step, carry):
            make(step)
            send(step - 1)
            return carry

        make(0)
        make(1)
        send(0, skip_own=True)
        lax.fori_loop(2, PLANE, stage, 0)
        if half == 1:
            combine(me, k)
            place[...] = pieces[k][me]
        send(PLANE - 1)

    for half in range(2):
        for k in range(2):
            if half == 0:
                all_of(landing[k], k).wait_recv()
            combine_half(half, k)

    def rows_of(block, k):
        start, height = PARTS[k]
        return pl.ds(pl.multiple_of(block * ROWS + start, FINE), height)

    def packed(block, k):
        height = PARTS[k][1]
        return pl.ds(pl.multiple_of(k * EARLY + block * height, FINE), height)

    def gram_part(rows, cols):
        product = lax.dot_general(
            x_bf[rows, :], x_bf[cols, :], (((1,), (1,)), ((), ())),
            preferred_element_type=jnp.float32,
        )
        part[rows, cols] = product.astype(jnp.bfloat16)

    def swap_part(rows, cols):
        at = (rows, cols)
        remote(part.at[at], other.at[at], 5, node, spot, 1 - core).start()

    early, late, full = pl.ds(0, EARLY), pl.ds(EARLY, FF - EARLY), pl.ds(0, FF)
    loads[1].wait()
    for k in range(2):
        all_of(pieces[k], 2 + k).wait_recv()

        def direction(block, carry, k=k):
            rows = rows_of(block, k)
            grad = decoded(near[rows, :])
            moment = momentum_beta * momentum[rows, :].astype(jnp.float32) + grad
            moment_out[rows, :] = moment.astype(jnp.bfloat16)
            ahead = grad + momentum_beta * moment
            nesterov[rows, :] = ahead
            x_bf[packed(block, k), :] = ahead.astype(jnp.bfloat16)
            return carry

        lax.fori_loop(0, PLANE, direction, 0, unroll=4)
        if k == 0:
            for i in range(EARLY // WIDE):
                gram_part(early, pl.ds(i * WIDE, WIDE))
            for i in range(EARLY // WIDE):
                swap_part(early, pl.ds(i * WIDE, WIDE))

    bands = [pl.ds(i * WIDE, WIDE) for i in range(FF // WIDE)]

    gram_part(full, late)
    gram_part(late, early)
    swap_part(full, late)
    eye = (CHIPS, CHIPS)
    on_diagonal = lax.broadcasted_iota(jnp.int32, eye, 0) == lax.broadcasted_iota(
        jnp.int32, eye, 1
    )

    def diagonal_of(ref):
        total = jnp.zeros(eye, jnp.float32)
        for i in range(FF // CHIPS):
            at = slice(i * CHIPS, (i + 1) * CHIPS)
            total += jnp.where(on_diagonal, ref[at, at].astype(jnp.float32), 0.0)
        return total

    diagonal = diagonal_of(part)
    swap_part(late, early)
    remote(part, other, 5, node, spot, 1 - core).wait_recv()
    diagonal += diagonal_of(other)
    squares = jnp.sum(jnp.sum(diagonal, axis=0, keepdims=True), axis=1, keepdims=True)
    scale = 1.0 / (jnp.sqrt(squares) + epsilon)
    scale_2 = scale * scale
    for cols in bands:
        both = part[:, cols].astype(jnp.float32) + other[:, cols].astype(jnp.float32)
        scaled = both * scale_2
        gram[:, cols] = scaled
        gram_bf[:, cols] = scaled.astype(jnp.bfloat16)

    for cols in bands:
        value = coef_b * gram[:, cols] + coef_c * mul(gram_bf[...], gram_bf[:, cols])
        first[:, cols] = value
        first_bf[:, cols] = value.astype(jnp.bfloat16)
    for cols in bands:
        half_way = coef_a * gram[:, cols] + mul(first_bf[...], gram_bf[:, cols])
        after = coef_a * half_way + mul(first_bf[...], half_way.astype(jnp.bfloat16))
        gram[:, cols] = after
        next_bf[:, cols] = after.astype(jnp.bfloat16)
    for cols in bands:
        second = coef_b * gram[:, cols] + coef_c * mul(next_bf[...], next_bf[:, cols])
        value = coef_a * (first[:, cols] + second)
        value += mul(first_bf[...], second.astype(jnp.bfloat16))
        both_bf[:, cols] = value.astype(jnp.bfloat16)

    loads[2].wait()
    length = step_scale * scale

    pairs = NODES // 2
    for i in (2, 1, 3, 0):
        pair = lax.rem(node // 2 + i, pairs)
        cols = pl.ds(pl.multiple_of(pair * WIDE, WIDE), WIDE)
        change[:, cols] = mul(both_bf[...], x_bf[:, cols])

        def update(block, carry, cols=cols):
            for k in range(2):
                rows = rows_of(block, k)
                iterate = (coef_a * coef_a) * nesterov[rows, cols]
                iterate += change[packed(block, k), cols]
                kept = (1.0 - learn_rate * weight_decay) * master[rows, cols]
                value = kept - length * iterate
                master_out[rows, cols] = value
                weights[rows, cols] = value.astype(jnp.bfloat16)
            return carry

        lax.fori_loop(0, PLANE, update, 0, unroll=4)

        def send_weights(step, carry, pair=pair):
            to_node = 2 * pair + lax.rem(node + step, 2)
            to_x = lax.rem(spot // 4 + lax.rem(step // 2, 4), 4)
            to_y = lax.rem(lax.rem(spot, 4) + step // 8, 4)
            to_spot = to_x * 4 + to_y
            block = part_of(weights, to_node, to_spot, 0)
            remote(block, arrived[0].at[me], 6, to_node, to_spot, core).start()
            return carry

        lax.fori_loop(1 if i == 0 else 0, 2 * PLANE, send_weights, 0)

    spread(weights, arrived[1], 1, 7)
    arrived[0][me] = part_of(weights, node, spot, 0)[...]

    for k in range(2):
        all_of(arrived[k], 6 + k).wait_recv()

        def choose(step, k=k):
            to_node, to_spot = partner(step, node, spot)
            chip = to_node * PLANE + to_spot
            chosen[k][chip] = arrived[k][owner_s[new_s[chip]]]

        deliver(choose, chosen[k], part_of(slots_out, node, spot, k), 8 + k)

    for k in range(2):
        all_of(chosen[k], 8 + k).wait_recv()
        for lane in (0, 2, 6, 8):
            all_of(chosen[k], lane + k).wait_send()
    remote(part, other, 5, node, spot, 1 - core).wait_send()


def write_kernel(moment_ref, master_ref, slots_ref, moment_out, master_out, slots_out, sems):
    copies = []
    for source, target in (
        (master_ref, master_out), (moment_ref, moment_out), (slots_ref, slots_out)
    ):
        for i in range(FF // WIDE):
            rows = pl.ds(i * WIDE, WIDE)
            sem = sems.at[len(copies)]
            copies.append(pltpu.make_async_copy(source.at[rows], target.at[0, rows], sem))
    for copy in copies:
        copy.start()
    for copy in copies:
        copy.wait()


def on_device(slot_grads, slot_tokens, old_slots, owner_chip, momentum, master, new_slots):
    bf, f32 = jnp.bfloat16, jnp.float32
    vmem = pl.BlockSpec(memory_space=pltpu.VMEM)
    smem = pl.BlockSpec(memory_space=pltpu.SMEM)
    hbm = pl.BlockSpec(memory_space=pl.ANY)
    matrix = (FF, HALF)
    square = (FF, FF)
    tall = (CHIPS, PARTS[0][1], COLS)
    low = (CHIPS, FINE, COLS)
    row = (1, CHIPS)
    kept = (pltpu.VMEM(matrix, bf), pltpu.VMEM(matrix, f32), pltpu.VMEM(matrix, bf))
    moment_new, master_new, slots = pl.pallas_call(
        step_kernel,
        out_shape=kept,
        in_specs=[hbm, vmem, vmem, vmem, hbm, hbm, smem, smem],
        out_specs=(vmem, vmem, vmem),
        scratch_shapes=[
            pltpu.VMEM(matrix, bf),
            pltpu.VMEM(matrix, bf),
            pltpu.VMEM(matrix, f32),
            pltpu.VMEM(tall, bf),
            pltpu.VMEM(low, bf),
            pltpu.VMEM(tall, bf),
            pltpu.VMEM(low, bf),
            pltpu.VMEM(matrix, bf),
            pltpu.VMEM(matrix, f32),
            pltpu.VMEM(matrix, bf),
            pltpu.VMEM(square, bf),
            pltpu.VMEM(square, bf),
            pltpu.VMEM(square, f32),
            pltpu.VMEM(square, bf),
            pltpu.VMEM(square, f32),
            pltpu.VMEM(square, bf),
            pltpu.VMEM(square, bf),
            pltpu.VMEM(square, bf),
            pltpu.VMEM(matrix, f32),
            pltpu.VMEM(matrix, bf),
            pltpu.VMEM(tall, bf),
            pltpu.VMEM(low, bf),
            pltpu.VMEM(tall, bf),
            pltpu.VMEM(low, bf),
            pltpu.VMEM((8, CHIPS), jnp.int32),
            pltpu.VMEM((8, CHIPS), f32),
            pltpu.SMEM((8, CHIPS), jnp.int32),
            pltpu.SMEM((8, CHIPS), f32),
            pltpu.SemaphoreType.DMA((5,)),
            pltpu.SemaphoreType.DMA((20,)),
        ],
        compiler_params=pltpu.CompilerParams(
            collective_id=0, has_side_effects=True, vmem_limit_bytes=50 * 2**20
        ),
    )(
        slot_grads,
        slot_tokens.reshape(row),
        old_slots.reshape(row),
        owner_chip.reshape(row),
        momentum,
        master,
        new_slots,
        owner_chip,
    )
    outs = tuple(jax.ShapeDtypeStruct((1, *matrix), kind) for kind in (bf, f32, bf))
    return pl.pallas_call(
        write_kernel,
        out_shape=outs,
        in_specs=[vmem, vmem, vmem],
        out_specs=(hbm, hbm, hbm),
        scratch_shapes=[pltpu.SemaphoreType.DMA((9,))],
        compiler_params=pltpu.CompilerParams(vmem_limit_bytes=2**20),
    )(moment_new, master_new, slots)


def solution(mesh):
    split = P(("node", "expert"), None, "column")
    return jax.shard_map(
        on_device,
        mesh=mesh,
        in_specs=(split, P(), P(), P(), split, split, P()),
        out_specs=(split, split, split),
        check_vma=False,
    )
```

```python
import math

import jax
import jax.numpy as jnp
from jax import lax
from jax.experimental import pallas as pl
from jax.experimental.pallas import tpu as pltpu
from jax.sharding import PartitionSpec as P

D = 2048
FF = 768
HALF = D // 2
CHIPS = 128
EXPERTS = 80
NODES = 8
PLANE = 16
ROWS = FF // PLANE
COLS = HALF // NODES
FINE = 16
PARTS = ((FINE, ROWS - FINE), (0, FINE))
WIDE = 256
EARLY = PLANE * PARTS[0][1]

coef_a = 3.4445
coef_b = -4.775
coef_c = 2.0315
momentum_beta = 0.95
learn_rate = 1.0
weight_decay = 0.1
epsilon = 1e-07
code_scale = 2.0**27
step_scale = learn_rate * 0.2 * math.sqrt(max(FF, D))

MESH = pl.DeviceIdType.MESH


def part_of(ref, node, spot, part):
    first, height = PARTS[part]
    rows = pl.ds(pl.multiple_of(spot * ROWS + first, FINE), height)
    cols = pl.ds(pl.multiple_of(node * COLS, COLS), COLS)
    return ref.at[rows, cols]


def coded(grad):
    large = grad * code_scale
    return ((large * large) * (large * jnp.abs(large))).astype(jnp.bfloat16)


def decoded(code):
    code = code.astype(jnp.float32)
    size = lax.rsqrt(lax.rsqrt(jnp.abs(code))) * (1.0 / code_scale)
    size = jnp.where(code == 0.0, 0.0, size)
    return jnp.where(code < 0.0, -size, size)


def mul(left, right):
    return jnp.dot(left, right, preferred_element_type=jnp.float32)


def tables(tokens_ref, old_ref, owner_ref, index_ref, weight_ref):
    shape = (CHIPS, CHIPS)
    across = lax.broadcasted_iota(jnp.int32, shape, 1)
    down = lax.broadcasted_iota(jnp.int32, shape, 0)
    owner = jnp.broadcast_to(owner_ref[...], shape).T
    match = (owner == across) & (down < EXPERTS)
    owned = jnp.sum(jnp.where(match, down + 1, 0), axis=0, keepdims=True) - 1
    old = jnp.broadcast_to(old_ref[...], shape).T
    tokens = jnp.broadcast_to(tokens_ref[...], shape).T
    picked = old == owned
    total = jnp.sum(jnp.where(picked, tokens, 0), axis=0, keepdims=True)
    total = jnp.maximum(total.astype(jnp.float32), 1.0)
    for k in range(4):
        first = jnp.min(jnp.where(picked, down, CHIPS), axis=0, keepdims=True)
        here = down == first
        count = jnp.sum(jnp.where(here, tokens, 0), axis=0, keepdims=True)
        weight_ref[k : k + 1, :] = count.astype(jnp.float32) / total
        index_ref[k : k + 1, :] = jnp.where(first < CHIPS, first, 0)
        picked = picked & jnp.logical_not(here)


def step_kernel(
    grads_ref, tokens_ref, old_ref, owner_ref, momentum_ref, master_ref, new_s, owner_s,
    moment_out, master_out, slots_out,
    local, momentum, master, landing_0, landing_1, pieces_0, pieces_1,
    near, nesterov, x_bf, part, other, gram, gram_bf, first, first_bf, next_bf, both_bf, change,
    weights, arrived_0, arrived_1, chosen_0, chosen_1,
    index_v, weight_v, index_s, weight_s, copy_sems, sems,
):
    node, spot, core = (lax.axis_index(a) for a in ("node", "expert", "column"))
    me = node * PLANE + spot
    landing, pieces = (landing_0, landing_1), (pieces_0, pieces_1)
    arrived, chosen = (arrived_0, arrived_1), (chosen_0, chosen_1)

    def remote(src, dst, lane, to_node, to_spot, to_core):
        return pltpu.make_async_remote_copy(
            src, dst, sems.at[2 * lane], sems.at[2 * lane + 1],
            device_id=(to_node, to_spot, to_core), device_id_type=MESH,
        )

    near_nodes = [lax.rem(node + by_node, NODES) for by_node in range(NODES)]

    def spot_at(step):
        to_x = lax.rem(spot // 4 + step // 4, 4)
        return to_x * 4 + lax.rem(lax.rem(spot, 4) + lax.rem(step, 4), 4)

    def every(body):
        for to_node in near_nodes[1:]:
            body(to_node, spot)

        def wrapped(step, carry):
            to_spot = spot_at(step)
            for to_node in near_nodes:
                body(to_node, to_spot)
            return carry

        lax.fori_loop(1, PLANE, wrapped, 0)

    def all_of(buffer, lane):
        rows = buffer.at[pl.ds(0, CHIPS - 1)]
        return remote(rows, rows, lane, node, spot, core)

    def spread(source, targets, k, lane):
        def send(to_node, to_spot):
            block = part_of(source, to_node, to_spot, k)
            remote(block, targets.at[me], lane, to_node, to_spot, core).start()

        every(send)
        targets[me] = part_of(source, node, spot, k)[...]

    def deliver(make, sources, place, lane):
        def make_step(step):
            to_spot = spot_at(step)
            for to_node in near_nodes:
                make(to_node * PLANE + to_spot)

        def send_step(step, nodes=near_nodes):
            to_spot = spot_at(step)
            for to_node in nodes:
                src = sources.at[to_node * PLANE + to_spot]
                remote(src, place, lane, to_node, to_spot, core).start()

        def stage(step, carry):
            make_step(step)
            send_step(step - 1)
            return carry

        make_step(0)
        make_step(1)
        send_step(0, near_nodes[1:])
        lax.fori_loop(2, PLANE, stage, 0)
        place[...] = sources[me]
        send_step(PLANE - 1)

    loads = (
        pltpu.make_async_copy(grads_ref.at[0], local, copy_sems.at[0]),
        pltpu.make_async_copy(momentum_ref.at[0], momentum, copy_sems.at[1]),
        pltpu.make_async_copy(master_ref.at[0], master, copy_sems.at[2]),
    )
    for load in loads:
        load.start()

    barrier = pltpu.get_barrier_semaphore()

    def greet(to_node, to_spot):
        pl.semaphore_signal(
            barrier, inc=1, device_id=(to_node, to_spot, core), device_id_type=MESH
        )

    every(greet)
    pl.semaphore_signal(barrier, inc=1, device_id=(node, spot, 1 - core), device_id_type=MESH)
    pl.semaphore_wait(barrier, CHIPS)
    loads[0].wait()
    for k in range(2):
        spread(local, landing[k], k, k)

    tables(tokens_ref, old_ref, owner_ref, index_v, weight_v)
    to_smem = (
        pltpu.make_async_copy(index_v, index_s, copy_sems.at[3]),
        pltpu.make_async_copy(weight_v, weight_s, copy_sems.at[4]),
    )
    for copy in to_smem:
        copy.start()
    for copy in to_smem:
        copy.wait()

    parity = lax.rem(node + spot // 4 + lax.rem(spot, 4), 2)

    def combine(chip, k):
        total = landing[k][index_s[0, chip]].astype(jnp.float32) * weight_s[0, chip]
        for j in range(1, 4):
            slot = landing[k][index_s[j, chip]].astype(jnp.float32)
            total += slot * weight_s[j, chip]
        pieces[k][chip] = coded(total)

    def combine_half(half, k):
        offset = lax.rem(parity + half, 2)
        place = part_of(near, node, spot, k)

        def chips_at(step):
            odd = lax.rem(offset + step // 4 + lax.rem(step, 4), 2)
            nodes = [lax.rem(node + odd + by_node, NODES) for by_node in range(0, NODES, 2)]
            return nodes, spot_at(step)

        def make(step):
            nodes, to_spot = chips_at(step)
            for to_node in nodes:
                combine(to_node * PLANE + to_spot, k)

        def send(step, skip_own=False):
            nodes, to_spot = chips_at(step)
            for i, to_node in enumerate(nodes):
                src = pieces[k].at[to_node * PLANE + to_spot]
                copy = remote(src, place, 2 + k, to_node, to_spot, core)
                if skip_own and i == 0:
                    pl.when(offset == 1)(copy.start)
                else:
                    copy.start()

        def stage(step, carry):
            make(step)
            send(step - 1)
            return carry

        make(0)
        make(1)
        send(0, skip_own=True)
        lax.fori_loop(2, PLANE, stage, 0)
        if half == 1:
            combine(me, k)
            place[...] = pieces[k][me]
        send(PLANE - 1)

    for half in range(2):
        for k in range(2):
            if half == 0:
                all_of(landing[k], k).wait_recv()
            combine_half(half, k)

    def rows_of(block, k):
        start, height = PARTS[k]
        return pl.ds(pl.multiple_of(block * ROWS + start, FINE), height)

    def packed(block, k):
        height = PARTS[k][1]
        return pl.ds(pl.multiple_of(k * EARLY + block * height, FINE), height)

    def gram_part(rows, cols):
        product = lax.dot_general(
            x_bf[rows, :], x_bf[cols, :], (((1,), (1,)), ((), ())),
            preferred_element_type=jnp.float32,
        )
        part[rows, cols] = product.astype(jnp.bfloat16)

    def swap_part(rows, cols):
        at = (rows, cols)
        remote(part.at[at], other.at[at], 5, node, spot, 1 - core).start()

    early, late, full = pl.ds(0, EARLY), pl.ds(EARLY, FF - EARLY), pl.ds(0, FF)
    loads[1].wait()
    for k in range(2):
        all_of(pieces[k], 2 + k).wait_recv()

        def direction(block, carry, k=k):
            rows = rows_of(block, k)
            grad = decoded(near[rows, :])
            moment = momentum_beta * momentum[rows, :].astype(jnp.float32) + grad
            moment_out[rows, :] = moment.astype(jnp.bfloat16)
            ahead = grad + momentum_beta * moment
            nesterov[rows, :] = ahead
            x_bf[packed(block, k), :] = ahead.astype(jnp.bfloat16)
            return carry

        lax.fori_loop(0, PLANE, direction, 0, unroll=4)
        if k == 0:
            for i in range(EARLY // WIDE):
                gram_part(early, pl.ds(i * WIDE, WIDE))
            for i in range(EARLY // WIDE):
                swap_part(early, pl.ds(i * WIDE, WIDE))

    bands = [pl.ds(i * WIDE, WIDE) for i in range(FF // WIDE)]

    gram_part(full, late)
    gram_part(late, early)
    swap_part(full, late)
    eye = (CHIPS, CHIPS)
    on_diagonal = lax.broadcasted_iota(jnp.int32, eye, 0) == lax.broadcasted_iota(
        jnp.int32, eye, 1
    )

    def diagonal_of(ref):
        total = jnp.zeros(eye, jnp.float32)
        for i in range(FF // CHIPS):
            at = slice(i * CHIPS, (i + 1) * CHIPS)
            total += jnp.where(on_diagonal, ref[at, at].astype(jnp.float32), 0.0)
        return total

    diagonal = diagonal_of(part)
    swap_part(late, early)
    remote(part, other, 5, node, spot, 1 - core).wait_recv()
    diagonal += diagonal_of(other)
    squares = jnp.sum(jnp.sum(diagonal, axis=0, keepdims=True), axis=1, keepdims=True)
    scale = 1.0 / (jnp.sqrt(squares) + epsilon)
    scale_2 = scale * scale
    for cols in bands:
        both = part[:, cols].astype(jnp.float32) + other[:, cols].astype(jnp.float32)
        scaled = both * scale_2
        gram[:, cols] = scaled
        gram_bf[:, cols] = scaled.astype(jnp.bfloat16)

    for cols in bands:
        value = coef_b * gram[:, cols] + coef_c * mul(gram_bf[...], gram_bf[:, cols])
        first[:, cols] = value
        first_bf[:, cols] = value.astype(jnp.bfloat16)
    for cols in bands:
        half_way = coef_a * gram[:, cols] + mul(first_bf[...], gram_bf[:, cols])
        after = coef_a * half_way + mul(first_bf[...], half_way.astype(jnp.bfloat16))
        gram[:, cols] = after
        next_bf[:, cols] = after.astype(jnp.bfloat16)
    for cols in bands:
        second = coef_b * gram[:, cols] + coef_c * mul(next_bf[...], next_bf[:, cols])
        value = coef_a * (first[:, cols] + second)
        value += mul(first_bf[...], second.astype(jnp.bfloat16))
        both_bf[:, cols] = value.astype(jnp.bfloat16)

    loads[2].wait()
    length = step_scale * scale

    pairs = NODES // 2
    for i in (2, 1, 3, 0):
        pair = lax.rem(node // 2 + i, pairs)
        cols = pl.ds(pl.multiple_of(pair * WIDE, WIDE), WIDE)
        change[:, cols] = mul(both_bf[...], x_bf[:, cols])

        def update(block, carry, cols=cols):
            for k in range(2):
                rows = rows_of(block, k)
                iterate = (coef_a * coef_a) * nesterov[rows, cols]
                iterate += change[packed(block, k), cols]
                kept = (1.0 - learn_rate * weight_decay) * master[rows, cols]
                value = kept - length * iterate
                master_out[rows, cols] = value
                weights[rows, cols] = value.astype(jnp.bfloat16)
            return carry

        lax.fori_loop(0, PLANE, update, 0, unroll=4)

        def send_weights(step, carry, pair=pair):
            to_node = 2 * pair + lax.rem(node + step, 2)
            to_x = lax.rem(spot // 4 + lax.rem(step // 2, 4), 4)
            to_y = lax.rem(lax.rem(spot, 4) + step // 8, 4)
            to_spot = to_x * 4 + to_y
            block = part_of(weights, to_node, to_spot, 0)
            remote(block, arrived[0].at[me], 6, to_node, to_spot, core).start()
            return carry

        lax.fori_loop(1 if i == 0 else 0, 2 * PLANE, send_weights, 0)

    spread(weights, arrived[1], 1, 7)
    arrived[0][me] = part_of(weights, node, spot, 0)[...]

    for k in range(2):
        all_of(arrived[k], 6 + k).wait_recv()

        def choose(chip, k=k):
            chosen[k][chip] = arrived[k][owner_s[new_s[chip]]]

        deliver(choose, chosen[k], part_of(slots_out, node, spot, k), 8 + k)

    for k in range(2):
        all_of(chosen[k], 8 + k).wait_recv()
        for lane in (0, 2, 6, 8):
            all_of(chosen[k], lane + k).wait_send()
    remote(part, other, 5, node, spot, 1 - core).wait_send()


def write_kernel(moment_ref, master_ref, slots_ref, moment_out, master_out, slots_out, sems):
    copies = []
    for source, target in (
        (master_ref, master_out), (moment_ref, moment_out), (slots_ref, slots_out)
    ):
        for i in range(FF // WIDE):
            rows = pl.ds(i * WIDE, WIDE)
            sem = sems.at[len(copies)]
            copies.append(pltpu.make_async_copy(source.at[rows], target.at[0, rows], sem))
    for copy in copies:
        copy.start()
    for copy in copies:
        copy.wait()


def on_device(slot_grads, slot_tokens, old_slots, owner_chip, momentum, master, new_slots):
    bf, f32 = jnp.bfloat16, jnp.float32
    vmem = pl.BlockSpec(memory_space=pltpu.VMEM)
    smem = pl.BlockSpec(memory_space=pltpu.SMEM)
    hbm = pl.BlockSpec(memory_space=pl.ANY)
    matrix = (FF, HALF)
    square = (FF, FF)
    tall = (CHIPS, PARTS[0][1], COLS)
    low = (CHIPS, FINE, COLS)
    row = (1, CHIPS)
    kept = (pltpu.VMEM(matrix, bf), pltpu.VMEM(matrix, f32), pltpu.VMEM(matrix, bf))
    moment_new, master_new, slots = pl.pallas_call(
        step_kernel,
        out_shape=kept,
        in_specs=[hbm, vmem, vmem, vmem, hbm, hbm, smem, smem],
        out_specs=(vmem, vmem, vmem),
        scratch_shapes=[
            pltpu.VMEM(matrix, bf),
            pltpu.VMEM(matrix, bf),
            pltpu.VMEM(matrix, f32),
            pltpu.VMEM(tall, bf),
            pltpu.VMEM(low, bf),
            pltpu.VMEM(tall, bf),
            pltpu.VMEM(low, bf),
            pltpu.VMEM(matrix, bf),
            pltpu.VMEM(matrix, f32),
            pltpu.VMEM(matrix, bf),
            pltpu.VMEM(square, bf),
            pltpu.VMEM(square, bf),
            pltpu.VMEM(square, f32),
            pltpu.VMEM(square, bf),
            pltpu.VMEM(square, f32),
            pltpu.VMEM(square, bf),
            pltpu.VMEM(square, bf),
            pltpu.VMEM(square, bf),
            pltpu.VMEM(matrix, f32),
            pltpu.VMEM(matrix, bf),
            pltpu.VMEM(tall, bf),
            pltpu.VMEM(low, bf),
            pltpu.VMEM(tall, bf),
            pltpu.VMEM(low, bf),
            pltpu.VMEM((8, CHIPS), jnp.int32),
            pltpu.VMEM((8, CHIPS), f32),
            pltpu.SMEM((8, CHIPS), jnp.int32),
            pltpu.SMEM((8, CHIPS), f32),
            pltpu.SemaphoreType.DMA((5,)),
            pltpu.SemaphoreType.DMA((20,)),
        ],
        compiler_params=pltpu.CompilerParams(
            collective_id=0, has_side_effects=True, vmem_limit_bytes=50 * 2**20
        ),
    )(
        slot_grads,
        slot_tokens.reshape(row),
        old_slots.reshape(row),
        owner_chip.reshape(row),
        momentum,
        master,
        new_slots,
        owner_chip,
    )
    outs = tuple(jax.ShapeDtypeStruct((1, *matrix), kind) for kind in (bf, f32, bf))
    return pl.pallas_call(
        write_kernel,
        out_shape=outs,
        in_specs=[vmem, vmem, vmem],
        out_specs=(hbm, hbm, hbm),
        scratch_shapes=[pltpu.SemaphoreType.DMA((9,))],
        compiler_params=pltpu.CompilerParams(vmem_limit_bytes=2**20),
    )(moment_new, master_new, slots)


def solution(mesh):
    split = P(("node", "expert"), None, "column")
    return jax.shard_map(
        on_device,
        mesh=mesh,
        in_specs=(split, P(), P(), P(), split, split, P()),
        out_specs=(split, split, split),
        check_vma=False,
    )
```
